32 devices in a mesh: rep: 2 (over x), dp: 16 (over y, z, core).
Axes of the slice: x: 2, y: 2, z: 4, core: 2. Of those that a mesh axis runs over, the one named last changes fastest.
Arguments:
- g_w_gate: bfloat16 [32, 2, 1280, 4480], P(('rep', 'dp')), parts along dimension 0
- g_w_up: bfloat16 [32, 2, 1280, 4480], P(('rep', 'dp')), parts along dimension 0
- g_w_down: bfloat16 [32, 2, 4480, 1280], P(('rep', 'dp')), parts along dimension 0
- w_gate: bfloat16 [2, 1280, 4480], replicated
- w_up: bfloat16 [2, 1280, 4480], replicated
- w_down: bfloat16 [2, 4480, 1280], replicated
- m_w_gate: float32 [2, 1280, 4480], P(None, 'dp')
- m_w_up: float32 [2, 1280, 4480], P(None, 'dp')
- m_w_down: float32 [2, 4480, 1280], P(None, 'dp')
- v_w_gate: float32 [2, 1280, 4480], P(None, 'dp')
- v_w_up: float32 [2, 1280, 4480], P(None, 'dp')
- v_w_down: float32 [2, 4480, 1280], P(None, 'dp')
Outputs:
- output 1: bfloat16 [4, 1280, 4480], P('rep'), parts along dimension 0
- output 2: bfloat16 [4, 1280, 4480], P('rep'), parts along dimension 0
- output 3: bfloat16 [4, 4480, 1280], P('rep'), parts along dimension 0
- output 4: float32 [4, 1280, 4480], P('rep', 'dp'), parts along dimension 0
- output 5: float32 [4, 1280, 4480], P('rep', 'dp'), parts along dimension 0
- output 6: float32 [4, 4480, 1280], P('rep', 'dp'), parts along dimension 0
- output 7: float32 [4, 1280, 4480], P('rep', 'dp'), parts along dimension 0
- output 8: float32 [4, 1280, 4480], P('rep', 'dp'), parts along dimension 0
- output 9: float32 [4, 4480, 1280], P('rep', 'dp'), parts along dimension 0
There are 2 independent parts. The reference program is written for one: setup_inputs(seed, part) draws one part's arguments, and reference() takes and returns one part's arrays. A program takes and returns all parts, laid end to end along the dimension named above; an argument that names none is the same for every part.
All inputs are finite; a program needn't handle non-finite values.
Results may differ from the reference program's by a relative error of at most 0.022.
Values are sent between devices in bfloat16 or wider.
A program may use at most 2 GiB of HBM per device.

```python
import jax
import jax.numpy as jnp
from jax import lax

DEVICES = 16
D = 1280
FF = 4480
LAYERS = 2
NAMES = ("w_gate", "w_up", "w_down")
SHAPES = {"w_gate": (LAYERS, D, FF), "w_up": (LAYERS, D, FF), "w_down": (LAYERS, FF, D)}


def setup_inputs(seed: int = 0, part: int = 0) -> dict:
    kz, *keys = jax.random.split(jax.random.key(seed), 1 + 5 * len(NAMES))
    loud = 2.0 ** jax.random.uniform(kz, (), jnp.float32, -1.0, 1.0)
    drawn = {}
    for name, key, both in zip(NAMES, keys[:3], keys[3:6], strict=True):
        own = jax.random.normal(jax.random.fold_in(key, part), (DEVICES, *SHAPES[name]), jnp.float32)
        shared = jax.random.normal(jax.random.fold_in(both, part), SHAPES[name], jnp.float32)
        drawn["g_" + name] = (loud * (0.7 * shared / DEVICES + 0.7 * own * DEVICES**-0.5)).astype(jnp.bfloat16)
    for name, key in zip(NAMES, keys[6:9], strict=True):
        drawn[name] = (jax.random.normal(key, SHAPES[name], jnp.float32) * SHAPES[name][1] ** -0.5).astype(jnp.bfloat16)
    for name, key in zip(NAMES, keys[9:12], strict=True):
        drawn["m_" + name] = loud * 0.5 * jax.random.normal(key, SHAPES[name], jnp.float32)
    for name, key in zip(NAMES, keys[12:15], strict=True):
        drawn["v_" + name] = loud * loud * jax.random.uniform(key, SHAPES[name], jnp.float32, 0.5, 1.5)
    return drawn


def adamw(w, m, v, g):
    m = 0.9 * m + 0.1 * g
    v = 0.95 * v + 0.05 * g * g
    step = m * lax.rsqrt(v + 1e-8) + 0.1 * w
    return (w - 0.02 * step).astype(jnp.bfloat16), m, v


def reference(g_w_gate, g_w_up, g_w_down, w_gate, w_up, w_down, m_w_gate, m_w_up, m_w_down, v_w_gate, v_w_up, v_w_down):
    def total(terms):
        return lax.scan(lambda so_far, term: (so_far + term.astype(jnp.float32), None), jnp.zeros(terms.shape[1:], jnp.float32), terms)[0]

    gradients = [total(terms).astype(jnp.bfloat16).astype(jnp.float32) for terms in (g_w_gate, g_w_up, g_w_down)]
    new = [
        adamw(w.astype(jnp.float32), m, v, g)
        for w, m, v, g in zip((w_gate, w_up, w_down), (m_w_gate, m_w_up, m_w_down), (v_w_gate, v_w_up, v_w_down), gradients, strict=True)
    ]
    return tuple(one[which] for which in range(3) for one in new)
```

```python
import functools

import jax
import jax.numpy as jnp
from jax import lax
from jax.experimental import pallas as pl
from jax.experimental.pallas import tpu as pltpu
from jax.sharding import PartitionSpec as P

F32, BF16 = jnp.float32, jnp.bfloat16
LANES = 128
H, HA, U = 400, 240, 80
D, S = 8, 4
SLABS = 2 * 4


def tiles(a):
    L, R, C = a.shape
    return a.reshape(L, R // 8, 8, C // LANES, LANES).transpose(0, 1, 3, 2, 4).reshape(L, R * C // LANES, LANES)


def untiles(a, shape):
    L, R, C = shape
    return a.reshape(L, R // 8, C // LANES, 8, LANES).transpose(0, 1, 3, 2, 4).reshape(L, R, C)


def kernel(R, Q, *refs):
    g, w, m, v = (refs[i : i + 3] for i in (0, 3, 6, 9))
    T, mo, vo = refs[12], refs[13:16], refs[16:19]
    (O, Pt, Ys, Yr, As, Ar, Bs, Br, Ybs, Ybr, wb, mb, vb, mn, vn, N) = refs[19:35]
    (oL, dS, dR, yS, yR, aS, aR, bS, bR, ybS, ybR, lw, lm, lv, sm, sv, sn, gaS, gaR, gbS, gbR, gyS, gyR, gzS, gzR, gdS, gdR) = refs[35:]
    HB = H - HA
    A, B = pl.ds(0, HA), pl.ds(HA, HB)
    rep, me = lax.axis_index("rep"), lax.axis_index("dp")
    y, z, c = me // 8, (me // 2) % 4, me % 2
    partner, across, right, left = me + 1 - 2 * c, me + 8 - 16 * y, me + 2, me - 2
    hops = (z, 3 - z)
    onward = (z < 3, z > 0)
    toward = (right, left)

    def remote(src, dst, ss, rs, to):
        return pltpu.make_async_remote_copy(src, dst, ss, rs, device_id=(rep, to), device_id_type=pl.DeviceIdType.MESH)

    def at(r):
        return r // Q, pl.multiple_of((r % Q) * H, 16)

    def ok(r):
        return jnp.logical_and(r >= 0, r < R)

    def add(n, out, *ins):
        def step(j, _):
            rows = pl.ds(pl.multiple_of(j * U, 8), U)
            acc = ins[0][rows].astype(F32)
            for x in ins[1:]:
                acc = acc + x[rows].astype(F32)
            out[rows] = acc.astype(BF16)
            return 0

        lax.fori_loop(0, n // U, step, 0)

    def own(r, k=0):
        wl, off = at(r)
        return pltpu.make_async_copy(g[k].at[wl % 2, :, :, c, pl.ds(off, H)], O.at[r % D], oL.at[r % D])

    def give(r, k=0):
        wl, off = at(r)
        return remote(g[k].at[wl % 2, :, :, 1 - c, pl.ds(off, H)], Pt.at[r % D], dS.at[r % D], dR.at[r % D], partner)

    def y_a(r):
        return remote(Ys.at[r % S], Yr.at[r % D], yS.at[r % D], yR.at[r % D], across)

    def z_a(r, b, side):
        return remote(As.at[side, r % S, b], Ar.at[side, r % D, b], aS.at[side, r % D, b], aR.at[side, r % D, b], toward[side])

    def z_b(r, b, side):
        return remote(Bs.at[side, r % S, b], Br.at[side, r % D, b], bS.at[side, r % D, b], bR.at[side, r % D, b], toward[side])

    def y_b(r):
        return remote(Ybs.at[r % S], Ybr.at[r % D], ybS.at[r % D], ybR.at[r % D], across)

    def loads(r, k=0):
        wl, off = at(r)
        s = r % S
        return (
            pltpu.make_async_copy(w[k].at[wl % 2, y, z, c, pl.ds(off, H)], wb.at[s], lw.at[s]),
            pltpu.make_async_copy(m[k].at[wl % 2, pl.ds(off, H)], mb.at[s], lm.at[s]),
            pltpu.make_async_copy(v[k].at[wl % 2, pl.ds(off, H)], vb.at[s], lv.at[s]),
        )

    def stores(r, k=0):
        wl, off = at(r)
        s = r % S
        return (
            pltpu.make_async_copy(mn.at[s], mo[k].at[wl % 2, pl.ds(off, H)], sm.at[s]),
            pltpu.make_async_copy(vn.at[s], vo[k].at[wl % 2, pl.ds(off, H)], sv.at[s]),
        )

    def keep(r):
        wl, off = at(r)
        return pltpu.make_async_copy(N.at[r % S], T.at[wl, y, z, c, pl.ds(off, H)], sn.at[r % S])

    def g_a(r, b, side, new=False):
        wl, off = at(r)
        here = T.at[wl, y, b, c, pl.ds(off, HA)]
        return remote(N.at[r % S, A] if new else here, here, gaS.at[side, r % D, b], gaR.at[side, r % D, b], toward[side])

    def g_yb(r):
        wl, off = at(r)
        return remote(N.at[r % S, B], T.at[wl, y, z, c, pl.ds(off + HA, HB)], gyS.at[r % D], gyR.at[r % D], across)

    def g_b(r, b, side):
        wl, off = at(r)
        here = T.at[wl, :, b, c, pl.ds(off + HA, HB)]
        return remote(here, here, gbS.at[side, r % D, b], gbR.at[side, r % D, b], toward[side])

    def g_ya(r):
        wl, off = at(r)
        here = T.at[wl, y, :, c, pl.ds(off, HA)]
        return remote(here, here, gzS.at[r % D], gzR.at[r % D], across)

    def g_d(r):
        wl, off = at(r)
        here = T.at[wl, :, :, c, pl.ds(off, H)]
        return remote(here, here, gdS.at[r % D], gdR.at[r % D], partner)

    def of_weight(r, fn):
        for k in range(3):
            pl.when(jnp.logical_and(ok(r), r // (2 * Q) == k))(functools.partial(fn, r, k))

    for side in range(2):

        @pl.when(jnp.logical_not(onward[1 - side]))
        def _():
            def zero(j, _):
                for x in (Ar, Br):
                    ref = x.at[side, j // 4, j % 4]
                    ref[...] = jnp.zeros(ref.shape, BF16)
                return 0

            lax.fori_loop(0, D * 4, zero, 0)

    barrier = pltpu.get_barrier_semaphore()
    for to, there in ((partner, True), (across, True), (right, z < 3), (left, z > 0)):

        @pl.when(there)
        def _():
            pl.semaphore_signal(barrier, inc=1, device_id=(rep, to), device_id_type=pl.DeviceIdType.MESH)

    inner = jnp.logical_and(z > 0, z < 3)
    pl.when(inner)(lambda: pl.semaphore_wait(barrier, 4))
    pl.when(jnp.logical_not(inner))(lambda: pl.semaphore_wait(barrier, 3))

    def iteration(i, _):
        def split(r, k):
            give(r, k).start()
            own(r, k).start()

        of_weight(i, split)

        r1 = i - 1

        @pl.when(ok(r1))
        def _():
            own(r1).wait()
            give(r1).wait_recv()
            s = r1 % D

            def block(b, _):
                add(HA, Ys.at[r1 % S, b], O.at[s, 1 - y, b, A], Pt.at[s, 1 - y, b, A])
                return 0

            lax.fori_loop(0, 4, block, 0)
            y_a(r1).start()

        for side in range(2):
            rb = i - 1 - hops[side]

            @pl.when(ok(rb))
            def _(rb=rb, side=side):
                s = rb % D

                def block(j, _):
                    b = 3 - j if side == 0 else j

                    @pl.when(hops[side] > 0)
                    def _():
                        z_b(rb, b, side).wait_recv()

                    @pl.when(b != z)
                    def _():
                        for yy in range(2):
                            add(HB, Bs.at[side, rb % S, b, yy], O.at[s, yy, b, B], Pt.at[s, yy, b, B], Br.at[side, s, b, yy])
                        z_b(rb, b, side).start()

                    return 0

                lax.fori_loop(0, 4 - hops[side], block, 0)

        r2 = i - 2

        @pl.when(ok(r2))
        def _():
            y_a(r2).wait_recv()

        for side in range(2):
            ra = i - 2 - hops[side]

            @pl.when(ok(ra))
            def _(ra=ra, side=side):
                s = ra % D

                def block(j, _):
                    b = 3 - j if side == 0 else j

                    @pl.when(hops[side] > 0)
                    def _():
                        z_a(ra, b, side).wait_recv()

                    @pl.when(b != z)
                    def _():
                        add(HA, As.at[side, ra % S, b], O.at[s, y, b, A], Pt.at[s, y, b, A], Yr.at[s, b], Ar.at[side, s, b])
                        z_a(ra, b, side).start()

                    return 0

                lax.fori_loop(0, 4 - hops[side], block, 0)

        of_weight(i - 3, lambda r, k: [x.start() for x in loads(r, k)] and None)

        r4 = i - 4

        @pl.when(ok(r4))
        def _():
            s = r4 % D
            add(HB, Ybs.at[r4 % S], O.at[s, 1 - y, z, B], Pt.at[s, 1 - y, z, B], Br.at[0, s, z, 1 - y], Br.at[1, s, z, 1 - y])
            y_b(r4).start()

        r5 = i - 5

        @pl.when(ok(r5))
        def _():
            s, t = r5 % D, r5 % S
            for x in loads(r5):
                x.wait()
            y_b(r5).wait_recv()

            def update(first, n, *ins):
                def step(j, _):
                    rows = pl.ds(pl.multiple_of(j * U, 8), U)
                    here = pl.ds(pl.multiple_of(first + j * U, 8), U)
                    total = ins[0][rows].astype(F32)
                    for x in ins[1:]:
                        total = total + x[rows].astype(F32)
                    grad = total.astype(BF16).astype(F32)
                    new_m = 0.9 * mb[t, here] + 0.1 * grad
                    new_v = 0.95 * vb[t, here] + 0.05 * grad * grad
                    old = wb[t, here].astype(F32)
                    mn[t, here] = new_m
                    vn[t, here] = new_v
                    N[t, here] = (old - 0.02 * (new_m * lax.rsqrt(new_v + 1e-8) + 0.1 * old)).astype(BF16)
                    return 0

                lax.fori_loop(0, n // U, step, 0)

            update(0, HA, O.at[s, y, z, A], Pt.at[s, y, z, A], Yr.at[s, z], Ar.at[0, s, z], Ar.at[1, s, z])
            update(HA, HB, O.at[s, y, z, B], Pt.at[s, y, z, B], Br.at[0, s, z, y], Br.at[1, s, z, y], Ybr.at[s])
            g_yb(r5).start()
            for side in range(2):
                pl.when(onward[side])(lambda side=side: g_a(r5, z, side, new=True).start())
            keep(r5).start()

        of_weight(r5, lambda r, k: [x.start() for x in stores(r, k)] and None)

        for d in range(1, 4):
            for side in range(2):
                r, b = i - 5 - d, (z - d, z + d)[side]

                @pl.when(jnp.logical_and(ok(r), hops[side] >= d))
                def _(r=r, b=b, side=side):
                    g_a(r, b, side).wait_recv()
                    pl.when(onward[side])(lambda: g_a(r, b, side).start())

        r6 = i - 6

        @pl.when(ok(r6))
        def _():
            keep(r6).wait()
            g_yb(r6).wait_recv()
            for side in range(2):
                pl.when(onward[side])(lambda side=side: g_b(r6, z, side).start())

        for d in range(1, 4):
            for side in range(2):
                r, b = i - 6 - d, (z - d, z + d)[side]

                @pl.when(jnp.logical_and(ok(r), hops[side] >= d))
                def _(r=r, b=b, side=side):
                    g_b(r, b, side).wait_recv()
                    pl.when(onward[side])(lambda: g_b(r, b, side).start())

        r8, r9, r10 = i - 8, i - 9, i - 10

        @pl.when(ok(r8))
        def _():
            g_ya(r8).start()

        @pl.when(ok(r9))
        def _():
            g_ya(r9).wait_recv()
            g_d(r9).start()

        @pl.when(ok(i - 2))
        def _():
            give(i - 2).wait_send()

        @pl.when(ok(i - 3))
        def _():
            y_a(i - 3).wait_send()

        @pl.when(ok(i - 6))
        def _():
            y_b(i - 6).wait_send()

        @pl.when(ok(i - 7))
        def _():
            g_yb(i - 7).wait_send()
            for x in stores(i - 7):
                x.wait()
            for side in range(2):
                pl.when(onward[side])(lambda side=side: g_a(i - 7, z, side).wait_send())

        @pl.when(ok(r8))
        def _():
            for side in range(2):
                pl.when(onward[side])(lambda side=side: g_b(r8, z, side).wait_send())

        @pl.when(ok(r10))
        def _():
            g_ya(r10).wait_send()
            g_d(r10).wait()

        for side in range(2):
            for copy, late in ((z_a, 4), (z_b, 3)):
                r = i - late - hops[side]

                @pl.when(ok(r))
                def _(r=r, side=side, copy=copy):
                    def block(j, _):
                        copy(r, 3 - j if side == 0 else j, side).wait_send()
                        return 0

                    lax.fori_loop(0, 3 - hops[side], block, 0)

            for d in range(1, 3):
                b = (z - d, z + d)[side]
                for copy, late in ((g_a, 7), (g_b, 8)):
                    r = i - late - d

                    @pl.when(jnp.logical_and(jnp.logical_and(ok(r), hops[side] >= d), onward[side]))
                    def _(r=r, b=b, side=side, copy=copy):
                        copy(r, b, side).wait_send()

        return 0

    lax.fori_loop(0, R + 10, iteration, 0)


def solution(mesh):
    def step(*arrays):
        terms, weights, m, v = (arrays[i : i + 3] for i in (0, 3, 6, 9))
        layers = m[0].shape[0]
        rows = m[0].shape[1] * m[0].shape[2] // LANES
        Q = rows // H
        R = 3 * layers * Q
        HB = H - HA
        whole = (layers, 2, 4, 2, rows, LANES)
        g = [tiles(t[0]).reshape(whole) for t in terms]
        w = [tiles(t).reshape(whole) for t in weights]
        dma, vmem = pltpu.SemaphoreType.DMA, pltpu.VMEM
        place = pl.BlockSpec(memory_space=pl.ANY)
        out = pl.pallas_call(
            functools.partial(kernel, R, Q),
            name="step",
            out_shape=[jax.ShapeDtypeStruct((3 * layers, *whole[1:]), BF16)] + [jax.ShapeDtypeStruct((layers, rows, LANES), F32)] * 6,
            in_specs=[place] * 12,
            out_specs=[place] * 7,
            scratch_shapes=[
                vmem((D, 2, 4, H, LANES), BF16),
                vmem((D, 2, 4, H, LANES), BF16),
                vmem((S, 4, HA, LANES), BF16),
                vmem((D, 4, HA, LANES), BF16),
                vmem((2, S, 4, HA, LANES), BF16),
                vmem((2, D, 4, HA, LANES), BF16),
                vmem((2, S, 4, 2, HB, LANES), BF16),
                vmem((2, D, 4, 2, HB, LANES), BF16),
                vmem((S, HB, LANES), BF16),
                vmem((D, HB, LANES), BF16),
                vmem((S, H, LANES), BF16),
                *[vmem((S, H, LANES), F32)] * 4,
                vmem((S, H, LANES), BF16),
                dma((D,)), dma((D,)), dma((D,)), dma((D,)), dma((D,)),
                dma((2, D, 4)), dma((2, D, 4)), dma((2, D, 4)), dma((2, D, 4)),
                dma((D,)), dma((D,)),
                dma((S,)), dma((S,)), dma((S,)), dma((S,)), dma((S,)), dma((S,)),
                dma((2, D, 4)), dma((2, D, 4)), dma((2, D, 4)), dma((2, D, 4)),
                dma((D,)), dma((D,)), dma((D,)), dma((D,)), dma((D,)), dma((D,)),
            ],
            compiler_params=pltpu.CompilerParams(collective_id=0, has_side_effects=True, vmem_limit_bytes=60 * 2**20),
        )(*g, *w, *(tiles(t) for t in (*m, *v)))
        gathered = [untiles(out[0][layers * k : layers * (k + 1)].reshape(layers, 16 * rows, LANES), t.shape) for k, t in enumerate(weights)]
        return (*gathered, *(untiles(o, t.shape) for o, t in zip(out[1:], (*m, *v), strict=True)))

    all_of, cut = P(None, None, None), P(None, "dp", None)
    return jax.shard_map(
        step,
        mesh=mesh,
        in_specs=(P(("rep", "dp"), None, None, None),) * 3 + (all_of,) * 3 + (cut,) * 6,
        out_specs=(P("rep", None, None),) * 3 + (P("rep", "dp", None),) * 6,
        check_vma=False,
    )
```

```python
import functools

import jax
import jax.numpy as jnp
from jax import lax
from jax.experimental import pallas as pl
from jax.experimental.pallas import tpu as pltpu
from jax.sharding import PartitionSpec as P


F32, BF16 = jnp.float32, jnp.bfloat16
LANES = 128
H, U = 200, 40
EVEN, SOME, LONE = 120, 144, 160
NF, NS = 10, 10
D, E, S, G = 8, 6, 3, 4
LIMIT1, LIMIT2 = 27 * 2**18, 27 * 2**18
TAIL = 6
FLOPS = 10**9
EARLY = 8
KEPT = 43


def tiles(a):
    L, R, C = a.shape
    return a.reshape(L, R // 8, 8, C // LANES, LANES).transpose(0, 1, 3, 2, 4).reshape(L, R * C // LANES, LANES)


def untiles(a, shape):
    L, R, C = shape
    return a.reshape(L, R // 8, C // LANES, 8, LANES).transpose(0, 1, 3, 2, 4).reshape(L, R, C)


def kernel(R, Q, *refs):
    g, w, m, v = (refs[i : i + 3] for i in (0, 3, 6, 9))
    T, V, mn, vn, L, O, Pt = refs[12:19]
    (Ys, Yr, As, Ar, Bs, Br, Ybs, Ybr, wb, mb, vb, N) = refs[19:31]
    (oL, dS, dR, yS, yR, aS, aR, bS, bR, ybS, ybR, lw, lm, lv, sn, gaS, gaR, gbS, gbR, gyS, gyR, gzS, gzR, gdS, gdR, bk) = refs[31:]
    RT = R - TAIL
    RV = RT - KEPT
    rep, me = lax.axis_index("rep"), lax.axis_index("dp")
    y, z, c = me // 8, (me // 2) % 4, me % 2
    partner, across, right, left = me + 1 - 2 * c, me + 8 - 16 * y, me + 2, me - 2
    hops = (z, 3 - z)
    onward = (z < 3, z > 0)
    toward = (right, left)

    def remote(src, dst, ss, rs, to):
        return pltpu.make_async_remote_copy(src, dst, ss, rs, device_id=(rep, to), device_id_type=pl.DeviceIdType.MESH)

    def at(r):
        return r // Q, pl.multiple_of((r % Q) * H, 8)

    def ok(r):
        return jnp.logical_and(r >= 0, r < R)

    def gathered(r):
        return jnp.logical_and(r >= 0, r < RT)

    def by_split(r, fn):
        for a, since, until in ((LONE, 0, NF), (SOME, NF, NS), (EVEN, NS, R)):
            if since < until:
                pl.when(jnp.logical_and(r >= since, r < until))(functools.partial(fn, a))

    def slot(b, side):
        return jnp.minimum(b, 2) if side else jnp.maximum(b - 1, 0)

    def far_first(j):
        return jnp.where(z < 2, 3 - j, j)

    def add(n, out, *ins):
        for first in range(0, n, U):
            rows = pl.ds(first, min(U, n - first))
            acc = ins[0][rows].astype(F32)
            for x in ins[1:]:
                acc = acc + x[rows].astype(F32)
            out[rows] = acc.astype(BF16)

    def own(r, k=0):
        wl, off = at(r)
        return pltpu.make_async_copy(g[k].at[wl % 2, :, :, c, pl.ds(off, H)], O.at[r % D], oL.at[r % G])

    def give(r, k=0):
        wl, off = at(r)
        return remote(g[k].at[wl % 2, :, :, 1 - c, pl.ds(off, H)], Pt.at[r % D], dS.at[r % G], dR.at[r % G], partner)

    def y_a(r, b, a):
        rows = pl.ds(0, a)
        return remote(Ys.at[r % S, b, rows], Yr.at[r % E, b, rows], yS.at[r % G], yR.at[r % D, b], across)

    def y_a_left(r, a):
        rows = pl.ds(0, a)
        return remote(Ys.at[r % S, :, rows], Yr.at[r % E, :, rows], yS.at[r % G], yR.at[r % D, 0], across)

    def z_a(r, b, side, a):
        j, rows = slot(b, side), pl.ds(0, a)
        return remote(As.at[side, r % S, j, rows], Ar.at[side, r % E, j, rows], aS.at[side, r % G], aR.at[side, r % G, j], toward[side])

    def z_a_left(r, n, side, a):
        some, rows = pl.ds(0, n), pl.ds(0, a)
        return remote(
            As.at[side, r % S, some, rows], Ar.at[side, r % E, some, rows], aS.at[side, r % G], aR.at[side, r % G, 0], toward[side]
        )

    def z_b(r, b, side, a):
        j, rows = slot(b, side), pl.ds(0, H - a)
        return remote(
            Bs.at[side, r % S, j, :, rows], Br.at[side, r % E, j, :, rows], bS.at[side, r % G], bR.at[side, r % G, j], toward[side]
        )

    def z_b_left(r, n, side, a):
        some, rows = pl.ds(0, n), pl.ds(0, H - a)
        return remote(
            Bs.at[side, r % S, some, :, rows], Br.at[side, r % E, some, :, rows], bS.at[side, r % G], bR.at[side, r % G, 0], toward[side]
        )

    def y_b(r, a):
        rows = pl.ds(0, H - a)
        return remote(Ybs.at[r % S, rows], Ybr.at[r % E, rows], ybS.at[r % G], ybR.at[r % G], across)

    def loads(r, k=0):
        wl, off = at(r)
        s = r % S
        return (
            pltpu.make_async_copy(w[k].at[wl % 2, y, z, c, pl.ds(off, H)], wb.at[s], lw.at[s]),
            pltpu.make_async_copy(m[k].at[wl % 2, pl.ds(off, H)], mb.at[s], lm.at[s]),
            pltpu.make_async_copy(v[k].at[wl % 2, pl.ds(off, H)], vb.at[s], lv.at[s]),
        )

    def new(r, kept, where, first, n):
        wl, off = at(r)
        if kept:
            return V.at[r - RV, *where, pl.ds(first, n)]
        return T.at[wl, *where, pl.ds(off + first, n)]

    def keep(r, kept=False, last=False):
        if last:
            return pltpu.make_async_copy(N.at[r % S], L.at[r - RT], sn.at[r % S])
        return pltpu.make_async_copy(N.at[r % S], new(r, kept, (y, z, c), 0, H), sn.at[r % S])

    def g_a(r, b, side, kept=False, mine=False):
        here = new(r, kept, (y, b, c), 0, EVEN)
        return remote(N.at[r % S, pl.ds(0, EVEN)] if mine else here, here, gaS.at[side, r % G, b - side], gaR.at[side, r % G, b - side], toward[side])

    def g_yb(r, kept=False):
        return remote(N.at[r % S, pl.ds(EVEN, H - EVEN)], new(r, kept, (y, z, c), EVEN, H - EVEN), gyS.at[r % G], gyR.at[r % G], across)

    def g_b(r, b, side, kept=False):
        here = new(r, kept, (slice(None), b, c), EVEN, H - EVEN)
        return remote(here, here, gbS.at[side, r % G, b - side], gbR.at[side, r % G, b - side], toward[side])

    def g_ya(r, kept=False):
        here = new(r, kept, (y, slice(None), c), 0, EVEN)
        return remote(here, here, gzS.at[r % G], gzR.at[r % G], across)

    def g_d(r, kept=False):
        here = new(r, kept, (slice(None), slice(None), c), 0, H)
        return remote(here, here, gdS.at[r % G], gdR.at[r % G], partner)

    def placed(r, fn):
        pl.when(r < RV)(lambda: fn(False))
        pl.when(r >= RV)(lambda: fn(True))

    def back(r):
        wl, off = at(r)
        s = (R + r) % D
        return [
            pltpu.make_async_copy(T.at[wl, :, :, core, pl.ds(off, H)], to.at[s], bk) for core, to in enumerate((O, Pt))
        ]

    def of_weight(r, fn):
        for k in range(3):
            pl.when(jnp.logical_and(ok(r), r // (2 * Q) == k))(functools.partial(fn, r, k))

    for side in range(2):

        @pl.when(jnp.logical_not(onward[1 - side]))
        def _():
            def zero(j, _):
                for x in (Ar, Br):
                    ref = x.at[side, j // 3, j % 3]
                    ref[...] = jnp.zeros(ref.shape, BF16)
                return 0

            lax.fori_loop(0, E * 3, zero, 0)

    barrier = pltpu.get_barrier_semaphore()
    for to, there in ((partner, True), (across, True), (right, z < 3), (left, z > 0)):

        @pl.when(there)
        def _():
            pl.semaphore_signal(barrier, inc=1, device_id=(rep, to), device_id_type=pl.DeviceIdType.MESH)

    inner = jnp.logical_and(z > 0, z < 3)
    pl.when(inner)(lambda: pl.semaphore_wait(barrier, 4))
    pl.when(jnp.logical_not(inner))(lambda: pl.semaphore_wait(barrier, 3))

    def iteration(i, _):
        def split(r, k):
            give(r, k).start()
            own(r, k).start()

        of_weight(i, split)

        early = i + 2 - R

        @pl.when(jnp.logical_and(early >= 0, early < EARLY))
        def _():
            for x in back(early):
                x.start()

        r1 = i - 1

        @pl.when(ok(r1))
        def _():
            own(r1).wait()
            give(r1).wait_recv()

        def start_y(a):
            s, rows = r1 % D, pl.ds(0, a)

            def block(j, _):
                b = far_first(j)
                add(a, Ys.at[r1 % S, b], O.at[s, 1 - y, b, rows], Pt.at[s, 1 - y, b, rows])
                y_a(r1, b, a).start()
                return 0

            lax.fori_loop(0, 4, block, 0)

        by_split(r1, start_y)

        def pass_on(side, copy, add_block):
            def block(j, _):
                b = 3 - j if side == 0 else j
                pl.when(hops[side] > 0)(lambda: copy(b).wait_recv())

                @pl.when(b != z)
                def _():
                    add_block(b, slot(b, side))
                    copy(b).start()

                return 0

            lax.fori_loop(0, 4 - hops[side], block, 0)

        for side in range(2):
            rb = i - 1 - hops[side]

            def both_rows(a, r=rb, side=side):
                s, e, rows = r % D, r % E, pl.ds(a, H - a)

                def add_block(b, j):
                    for yy in range(2):
                        add(H - a, Bs.at[side, r % S, j, yy], O.at[s, yy, b, rows], Pt.at[s, yy, b, rows], Br.at[side, e, j, yy])

                pass_on(side, lambda b: z_b(r, b, side, a), add_block)

            by_split(rb, both_rows)

        for side in range(2):
            ra = i - 2 - hops[side]

            def one_row(a, r=ra, side=side):
                s, e, rows = r % D, r % E, pl.ds(0, a)

                def add_block(b, j):
                    y_a(r, b, a).wait_recv()
                    add(a, As.at[side, r % S, j], O.at[s, y, b, rows], Pt.at[s, y, b, rows], Yr.at[e, b], Ar.at[side, e, j])

                pass_on(side, lambda b: z_a(r, b, side, a), add_block)

            by_split(ra, one_row)

        of_weight(i - 3, lambda r, k: [x.start() for x in loads(r, k)] and None)

        r4 = i - 4

        def start_yb(a):
            s, e, rows = r4 % D, r4 % E, pl.ds(a, H - a)
            far = [Br.at[side, e, slot(z, side), 1 - y] for side in range(2)]
            add(H - a, Ybs.at[r4 % S], O.at[s, 1 - y, z, rows], Pt.at[s, 1 - y, z, rows], *far)
            y_b(r4, a).start()

        by_split(r4, start_yb)

        r5 = i - 5

        def update(a):
            s, e, t = r5 % D, r5 % E, r5 % S
            wl, off = at(r5)
            for x in loads(r5):
                x.wait()
            y_a(r5, z, a).wait_recv()
            y_b(r5, a).wait_recv()

            def rows_of(first, n, *ins):
                for start in range(0, n, U):
                    size = min(U, n - start)
                    rows, here = pl.ds(start, size), pl.ds(first + start, size)
                    there = pl.ds(pl.multiple_of(off + first + start, 8), size)
                    total = ins[0][rows].astype(F32)
                    for x in ins[1:]:
                        total = total + x[rows].astype(F32)
                    grad = total.astype(BF16).astype(F32)
                    new_m = 0.9 * mb[t, here] + 0.1 * grad
                    new_v = 0.95 * vb[t, here] + 0.05 * grad * grad
                    old = wb[t, here].astype(F32)
                    mn[wl, there] = new_m
                    vn[wl, there] = new_v
                    N[t, here] = (old - 0.02 * (new_m * lax.rsqrt(new_v + 1e-8) + 0.1 * old)).astype(BF16)

            A, B = pl.ds(0, a), pl.ds(a, H - a)
            sums = [[x.at[side, e, slot(z, side)] for side in range(2)] for x in (Ar, Br)]
            rows_of(0, a, O.at[s, y, z, A], Pt.at[s, y, z, A], Yr.at[e, z], *sums[0])
            rows_of(a, H - a, O.at[s, y, z, B], Pt.at[s, y, z, B], *(x.at[y] for x in sums[1]), Ybr.at[e])

        by_split(r5, update)

        @pl.when(ok(r5))
        def _():
            def send(kept):
                g_yb(r5, kept).start()
                for side in range(2):
                    pl.when(onward[side])(lambda side=side: g_a(r5, z, side, kept, mine=True).start())
                keep(r5, kept).start()

            @pl.when(r5 < RT)
            def _():
                placed(r5, send)

            @pl.when(r5 >= RT)
            def _():
                keep(r5, last=True).start()

        for d in range(1, 4):
            for side in range(2):
                r, b = i - 5 - d, (z - d, z + d)[side]

                @pl.when(jnp.logical_and(gathered(r), hops[side] >= d))
                def _(r=r, b=b, side=side):
                    g_a(r, b, side).wait_recv()
                    pl.when(onward[side])(lambda: placed(r, lambda kept: g_a(r, b, side, kept).start()))

        r6 = i - 6

        @pl.when(ok(r6))
        def _():
            keep(r6).wait()

        @pl.when(gathered(r6))
        def _():
            g_yb(r6).wait_recv()
            for side in range(2):
                pl.when(onward[side])(lambda side=side: placed(r6, lambda kept: g_b(r6, z, side, kept).start()))

        for d in range(1, 4):
            for side in range(2):
                r, b = i - 6 - d, (z - d, z + d)[side]

                @pl.when(jnp.logical_and(gathered(r), hops[side] >= d))
                def _(r=r, b=b, side=side):
                    g_b(r, b, side).wait_recv()
                    pl.when(onward[side])(lambda: placed(r, lambda kept: g_b(r, b, side, kept).start()))

        r8, r9, r10 = i - 8, i - 9, i - 10

        @pl.when(gathered(r8))
        def _():
            placed(r8, lambda kept: g_ya(r8, kept).start())

        @pl.when(gathered(r9))
        def _():
            g_ya(r9).wait_recv()
            placed(r9, lambda kept: g_d(r9, kept).start())

        @pl.when(ok(i - 2))
        def _():
            give(i - 2).wait_send()

        by_split(i - 3, lambda a: y_a_left(i - 3, a).wait_send())

        by_split(i - 6, lambda a: y_b(i - 6, a).wait_send())

        @pl.when(gathered(i - 7))
        def _():
            g_yb(i - 7).wait_send()
            for side in range(2):
                pl.when(onward[side])(lambda side=side: g_a(i - 7, z, side).wait_send())

        @pl.when(gathered(r8))
        def _():
            for side in range(2):
                pl.when(onward[side])(lambda side=side: g_b(r8, z, side).wait_send())

        @pl.when(gathered(r10))
        def _():
            g_ya(r10).wait_send()
            g_d(r10).wait()

        for side in range(2):
            for copies, late in ((z_a_left, 4), (z_b_left, 3)):
                r = i - late - hops[side]

                def sent(a, r=r, side=side, copies=copies):
                    for n in range(1, 4):
                        pl.when(hops[side] == 3 - n)(lambda n=n: copies(r, n, side, a).wait_send())

                by_split(r, sent)

            for d in range(1, 3):
                b = (z - d, z + d)[side]
                for copy, late in ((g_a, 7), (g_b, 8)):
                    r = i - late - d

                    @pl.when(jnp.logical_and(jnp.logical_and(gathered(r), hops[side] >= d), onward[side]))
                    def _(r=r, b=b, side=side, copy=copy):
                        copy(r, b, side).wait_send()

        return 0

    lax.fori_loop(0, max(R + 6, RT + 10), iteration, 0)
    early = V.at[pl.ds(0, EARLY)]
    pltpu.make_async_copy(early, early, bk).wait()


def finish(R, Q, k, *refs):
    T, V, mn, vn, O, Pt, whole, m, v, buf, inS, outS, vS, mS, bk = refs
    RT = R - TAIL
    RV = RT - KEPT
    F = buf.shape[0]
    first, last = 2 * k * Q, min(2 * (k + 1) * Q, RT)
    near = min(max(RV, first), last)
    far = max(first, EARLY)

    def at(r):
        return r // Q, pl.multiple_of((r % Q) * H, 8)

    def load(r):
        wl, off = at(r)
        return pltpu.make_async_copy(T.at[wl, :, :, :, pl.ds(off, H)], buf.at[r % F], inS.at[r % F])

    def store(r, kept=False):
        wl, off = at(r)
        src, sem = (V.at[r - RV], vS) if kept else (buf.at[r % F], outS.at[r % F])
        return pltpu.make_async_copy(src, whole.at[wl % 2, :, :, :, pl.ds(off, H)], sem)

    def each(lo, hi, fn):
        lax.fori_loop(lo, hi, lambda r, _: (fn(r), 0)[1], 0)

    ahead = F // 2 + 1
    each(far, min(far + ahead, near), lambda r: load(r).start())
    moments = [pltpu.make_async_copy(x.at[pl.ds(2 * k, 2)], o, mS.at[j]) for j, (x, o) in enumerate(((mn, m), (vn, v)))]
    for x in moments:
        x.start()
    each(near, last, lambda r: store(r, True).start())

    def early(r):
        wl, off = at(r)
        for core, x in enumerate((O, Pt)):
            pltpu.make_async_copy(x.at[(R + r) % D], whole.at[wl % 2, :, :, core, pl.ds(off, H)], bk).start()

    each(first, far, early)

    def move(r):
        load(r).wait()
        store(r).start()

        @pl.when(r + ahead < near)
        def _():
            pl.when(r + ahead >= far + F)(lambda: store(r + ahead - F).wait())
            load(r + ahead).start()

    each(far, near, move)
    each(max(far, near - F), near, lambda r: store(r).wait())
    if first < far:
        stored = V.at[pl.ds(0, far - first)]
        pltpu.make_async_copy(stored, stored, bk).wait()
    if near < last:
        stored = V.at[pl.ds(near - RV, last - near)]
        pltpu.make_async_copy(stored, stored, vS).wait()
    for x in moments:
        x.wait()


def place_tail(R, Q, *refs):
    parts, out, buf, inS, outS = refs[1:17], refs[17], *refs[18:]
    RT = R - TAIL
    me = lax.axis_index("dp")
    y, z, c = me // 8, (me // 2) % 4, me % 2
    off, layer = (RT % Q) * H, (RT // Q) % 2
    loads = [pltpu.make_async_copy(p, buf.at[j], inS.at[j]) for j, p in enumerate(parts)]
    for x in loads:
        x.start()
    for j in range(16):
        core, across, d = j // 8, (j // 4) % 2, j % 4
        yy, cc = (1 - y if across else y), (1 - c if core else c)
        loads[j].wait()
        x = pltpu.make_async_copy(buf.at[j], out.at[layer, yy, (z + 4 - d) % 4, cc, pl.ds(off, TAIL * H)], outS)
        x.start()
    pltpu.make_async_copy(buf, buf, outS).wait()


def solution(mesh):
    def inside(*arrays):
        terms, weights, m, v = (arrays[i : i + 3] for i in (0, 3, 6, 9))
        layers = m[0].shape[0]
        rows = m[0].shape[1] * m[0].shape[2] // LANES
        Q = rows // H
        R = 3 * layers * Q
        HA, HB = max(EVEN, LONE), H - EVEN
        whole = (layers, 2, 4, 2, rows, LANES)
        g = [tiles(t[0]).reshape(whole) for t in terms]
        w = [tiles(t).reshape(whole) for t in weights]
        dma, vmem = pltpu.SemaphoreType.DMA, pltpu.VMEM
        hbm = pl.BlockSpec(memory_space=pltpu.HBM)
        near = pl.BlockSpec(memory_space=pltpu.VMEM)
        like = [
            jax.ShapeDtypeStruct((3 * layers, *whole[1:]), BF16),
            vmem((KEPT, 2, 4, 2, H, LANES), BF16),
            *[vmem((3 * layers, rows, LANES), F32)] * 2,
            jax.ShapeDtypeStruct((TAIL, H, LANES), BF16),
            *[vmem((D, 2, 4, H, LANES), BF16)] * 2,
        ]
        mid = pl.pallas_call(
            functools.partial(kernel, R, Q),
            name="step",
            out_shape=like,
            in_specs=[hbm] * 12,
            out_specs=[hbm, near, near, near, hbm, near, near],
            scratch_shapes=[
                vmem((S, 4, HA, LANES), BF16),
                vmem((E, 4, HA, LANES), BF16),
                vmem((2, S, 3, HA, LANES), BF16),
                vmem((2, E, 3, HA, LANES), BF16),
                vmem((2, S, 3, 2, HB, LANES), BF16),
                vmem((2, E, 3, 2, HB, LANES), BF16),
                vmem((S, HB, LANES), BF16),
                vmem((E, HB, LANES), BF16),
                vmem((S, H, LANES), BF16),
                *[vmem((S, H, LANES), F32)] * 2,
                vmem((S, H, LANES), BF16),
                *[dma((G,))] * 4,
                dma((D, 4)),
                *[dma((2, G)), dma((2, G, 3))] * 2,
                *[dma((G,))] * 2,
                *[dma((S,))] * 4,
                *[dma((2, G, 3))] * 4,
                *[dma((G,))] * 6,
                dma(()),
            ],
            compiler_params=pltpu.CompilerParams(collective_id=0, has_side_effects=True, vmem_limit_bytes=LIMIT1),
        )(*g, *w, *(pltpu.with_memory_space_constraint(tiles(t), pltpu.HBM) for t in (*m, *v)))
        T, *kept = mid[:4]
        kept += mid[5:]
        kept = [pltpu.with_memory_space_constraint(x, pltpu.VMEM) for x in kept]

        def shift(x, to):
            places = [(y, z, c) for y in range(2) for z in range(4) for c in range(2)]
            number = lambda y, z, c: (y * 4 + z) * 2 + c
            return lax.ppermute(x, "dp", [(number(*p), number(*to(*p))) for p in places])

        def along(x, d):
            return shift(x, lambda y, z, c: (y, (z + d) % 4, c))

        def across(x):
            return shift(x, lambda y, z, c: (1 - y, z, c))

        def other(x):
            return shift(x, lambda y, z, c: (y, z, 1 - c))

        F = 8

        def finished(k):
            return pl.pallas_call(
                functools.partial(finish, R, Q, k),
                out_shape=[pltpu.HBM(whole, BF16)] + [pltpu.HBM((layers, rows, LANES), F32)] * 2,
                in_specs=[hbm, *[near] * 5],
                out_specs=[hbm] * 3,
                scratch_shapes=[vmem((F, 2, 4, 2, H, LANES), BF16), dma((F,)), dma((F,)), dma(()), dma((2,)), dma(())],
                compiler_params=pltpu.CompilerParams(vmem_limit_bytes=LIMIT2),
                cost_estimate=pl.CostEstimate(flops=FLOPS, bytes_accessed=6 * 10**7, transcendentals=0),
            )(T, *kept)

        def after(one, xs):
            moment, *xs = lax.optimization_barrier((one[1], *xs))
            return [one[0], moment, one[2]], xs

        mine = mid[4].reshape(TAIL * H, LANES)
        row = [mine, *(along(mine, d) for d in (1, 2, 3))]
        there = [across(mine)]
        done = [finished(0)]
        done[0], (x1,) = after(done[0], row[1:2])
        there.append(across(x1))
        done.append(finished(2))
        done[1], ready = after(done[1], (*row, *there))
        there += [across(x) for x in ready[2:4]]
        second = []
        for x in ready:
            second.append(other(x))
        done.append(finished(1))
        done[2], ready = after(done[2], there[2:])
        second += [other(x) for x in ready]
        parts = (*row, *there, *second)
        new_w, new_m, new_v = ([done[k][j] for k in (0, 2, 1)] for j in range(3))
        new_w[2] = pl.pallas_call(
            functools.partial(place_tail, R, Q),
            name="tail",
            out_shape=jax.ShapeDtypeStruct(whole, BF16),
            in_specs=[hbm, *[pl.BlockSpec(memory_space=pl.ANY)] * 16],
            out_specs=hbm,
            scratch_shapes=[vmem((16, TAIL * H, LANES), BF16), dma((16,)), dma(())],
            input_output_aliases={0: 0},
            compiler_params=pltpu.CompilerParams(vmem_limit_bytes=LIMIT2),
        )(new_w[2], *parts)
        weights_out = [untiles(o.reshape(layers, 16 * rows, LANES), t.shape) for o, t in zip(new_w, weights, strict=True)]
        return (*weights_out, *(untiles(o, t.shape) for o, t in zip((*new_m, *new_v), (*m, *v), strict=True)))

    all_of, cut = P(None, None, None), P(None, "dp", None)
    return jax.shard_map(
        inside,
        mesh=mesh,
        in_specs=(P(("rep", "dp"), None, None, None),) * 3 + (all_of,) * 3 + (cut,) * 6,
        out_specs=(P("rep", None, None),) * 3 + (P("rep", "dp", None),) * 6,
        check_vma=False,
    )
```
